32 devices in a mesh: seq: 2 (over x), row: 4 (over y, core), col: 4 (over z).
Axes of the slice: x: 2, y: 2, z: 4, core: 2. Of those that a mesh axis runs over, the one named last changes fastest.
Arguments:
- activations: bfloat16 [2, 64, 8192], P(None, 'row', 'seq'), may hold values from -6 to 6
- gradients: bfloat16 [2, 64, 8192], P(None, 'col', 'seq'), may hold values from -6 to 6
- basis_in: bfloat16 [8192, 4096], P('seq', 'col'), may hold values from -0.0625 to 0.0625
- basis_out: bfloat16 [8192, 4096], P('seq', 'row'), may hold values from -0.0625 to 0.0625
- lengths: int32 [2], replicated, may hold values from 16 to 64
Outputs:
- corrections: float32 [4096, 4096], P(('row', 'seq'), 'col')
The draws below stay inside these ranges and needn't reach their ends.
All inputs are finite; a program needn't handle non-finite values.
Results may differ from the reference program's by a relative error of at most 0.0023.
Values may be sent and summed in bfloat16 or wider, within the bound.
No kernel may reach another device: no remote copies, remote signals or barrier semaphores. Data moves between devices by JAX's collectives and lax.ppermute only.
A program may use at most 64 MiB of HBM per device.

```python
import jax
import jax.numpy as jnp
from jax import lax

FEAT_IN = 8192
FEAT_OUT = 8192
DIRS_IN = 4096
DIRS_OUT = 4096
MAXLEN = 64
SEQS = 2


def steps_of(own_key, dims, split, smallest, high):
    def one(position, blocks):
        steps = jax.random.uniform(jax.random.fold_in(jax.random.fold_in(own_key, 6), position), (blocks,), jnp.float32, smallest / len(split), high / len(split))
        return jnp.repeat(jnp.exp(steps), dims[position] // blocks).reshape((-1,) + (1,) * (len(dims) - position - 1))

    loudness = one(*split[0])
    for cut in split[1:]:
        loudness = loudness * one(*cut)
    return loudness


def normal_values(rng, dims, deviation, bound, cuts=(), held_as=jnp.bfloat16):
    level = steps_of(rng, dims, cuts, -0.22, 0.18) if cuts else 1.0
    result = jax.random.normal(rng, dims, jnp.float32) * deviation * level
    return jnp.minimum(jnp.maximum(result, -bound), bound).astype(held_as)


def setup_inputs(seed: int = 0) -> dict:
    keys = jax.random.split(jax.random.key(seed), 6)
    return {
        "activations": normal_values(keys[0], (SEQS, MAXLEN, FEAT_IN), 1.0, 6.0, ((1, 4), (2, 2))),
        "gradients": normal_values(keys[1], (SEQS, MAXLEN, FEAT_OUT), 1.0, 6.0, ((1, 4), (2, 2))),
        "basis_in": normal_values(keys[2], (FEAT_IN, DIRS_IN), FEAT_IN ** -0.5, 0.0625, ((0, 2), (1, 4))),
        "basis_out": normal_values(keys[3], (FEAT_OUT, DIRS_OUT), FEAT_OUT ** -0.5, 0.0625, ((0, 2), (1, 4))),
        "lengths": jax.random.randint(keys[4], (SEQS,), MAXLEN // 4, MAXLEN + 1).astype(jnp.int32),
    }


def reference(activations, gradients, basis_in, basis_out, lengths):
    slots = jnp.arange(MAXLEN).astype(jnp.int32)

    def one_sequence(total, index):
        turned_in = jnp.dot(activations[index], basis_in, preferred_element_type=jnp.float32).astype(jnp.bfloat16)
        turned_out = jnp.dot(gradients[index], basis_out, preferred_element_type=jnp.float32).astype(jnp.bfloat16)
        live_rows = slots < lengths[index]
        kept = jnp.where(live_rows[:, None], turned_out, jnp.zeros((), jnp.bfloat16))
        product_tile = lax.dot_general(kept, turned_in, (((0,), (0,)), ((), ())), preferred_element_type=jnp.float32)
        return total + product_tile * product_tile, None

    start_total = jnp.zeros((DIRS_OUT, DIRS_IN), jnp.float32)
    total, unused = lax.scan(one_sequence, start_total, jnp.arange(SEQS).astype(jnp.int32))
    return total / (SEQS * MAXLEN)
```

```python
import jax
import jax.numpy as jnp
from jax import lax
from jax.sharding import PartitionSpec as P


def turned_terms(tokens, basis):
    return jnp.einsum("ntf,fk->ntk", tokens, basis, preferred_element_type=jnp.float32)


def shifted(size, step):
    if size & (size - 1) == 0:
        return [(i, i ^ step) for i in range(size)]
    return [(i, (i + step) % size) for i in range(size)]


def sources(size, own, step):
    return own ^ step if size & (size - 1) == 0 else (own - step) % size


def every_token(turned, axis):
    size = lax.axis_size(axis)
    own = lax.axis_index(axis)
    seqs, tokens, dirs = turned.shape
    whole = jnp.zeros((seqs, size * tokens, dirs), turned.dtype)
    pieces = [turned] + [lax.ppermute(turned, axis, shifted(size, k)) for k in range(1, size)]
    for k, piece in enumerate(pieces):
        whole = lax.dynamic_update_slice(whole, piece, (0, sources(size, own, k) * tokens, 0))
    return whole


def summed_half(terms, axis):
    size = lax.axis_size(axis)
    own = lax.axis_index(axis)
    width = terms.shape[2] // size

    def part(owner):
        return lax.dynamic_slice_in_dim(terms, owner * width, width, 2)

    total = part(own)
    for k in range(1, size):
        if size & (size - 1) == 0:
            target = own ^ k
        else:
            target = (own + k) % size
        total = total + lax.ppermute(part(target), axis, shifted(size, k))
    return total


def summed_whole(terms, axis):
    if lax.axis_size(axis) > 2:
        return lax.psum(terms, axis)
    return terms + lax.ppermute(terms, axis, shifted(2, 1))


def local(activations, gradients, basis_in, basis_out, lengths):
    seqs = activations.shape[0]
    slot_total = gradients.shape[1] * lax.axis_size("col")
    turned_out = summed_half(turned_terms(gradients, basis_out), "seq").astype(jnp.bfloat16)
    turned_in = summed_whole(turned_terms(activations, basis_in), "seq").astype(jnp.bfloat16)
    slots = lax.axis_index("col") * gradients.shape[1] + jnp.arange(gradients.shape[1])
    live = slots[None, :] < lengths[:, None]
    kept = jnp.where(live[:, :, None], turned_out, jnp.zeros((), jnp.bfloat16))
    every_out = every_token(kept, "col")
    every_in = every_token(turned_in, "row")
    total = 0.0
    for n in range(seqs):
        tile = lax.dot_general(
            every_out[n], every_in[n], (((0,), (0,)), ((), ())), preferred_element_type=jnp.float32
        )
        total = total + tile * tile
    return total / (seqs * slot_total)


def solution(mesh):
    return jax.shard_map(
        local,
        mesh=mesh,
        in_specs=(
            P(None, "row", "seq"),
            P(None, "col", "seq"),
            P("seq", "col"),
            P("seq", "row"),
            P(),
        ),
        out_specs=P(("row", "seq"), "col"),
        check_vma=False,
    )
```

```python
import functools

import jax
import jax.numpy as jnp
from jax import lax
from jax.experimental import pallas as pl
from jax.experimental.pallas import tpu as pltpu
from jax.sharding import PartitionSpec as P


CHUNKS = 8


def turning_kernel(*refs):
    pairs = len(refs) // 7
    sources, terms, scratch = refs[: 2 * pairs], refs[2 * pairs : 3 * pairs], refs[3 * pairs :]
    jobs = []
    for p in range(pairs):
        tokens_hbm, basis_hbm = sources[2 * p : 2 * p + 2]
        tokens, basis, token_sem, basis_sems = scratch[4 * p : 4 * p + 4]
        count, rows, _ = basis.shape
        loads = [pltpu.make_async_copy(tokens_hbm, tokens, token_sem)]
        for k in range(count):
            loads.append(
                pltpu.make_async_copy(
                    basis_hbm.at[pl.ds(k * rows, rows)], basis.at[k], basis_sems.at[k]
                )
            )
        jobs.append(loads)
    for p, loads in enumerate(jobs):
        for k, load in enumerate(loads):
            load.start(priority=int(p > 0) if pairs > 1 else int(2 * k > len(loads)))
    for p, loads in enumerate(jobs):
        tokens, basis = scratch[4 * p : 4 * p + 2]
        count, rows, _ = basis.shape
        loads[0].wait()
        total = None
        for k in range(count):
            loads[k + 1].wait()
            part = jnp.dot(
                tokens[:, k * rows : (k + 1) * rows], basis[k], preferred_element_type=jnp.float32
            )
            total = part if total is None else total + part
        terms[p][...] = total


def turned_terms(*pairs):
    shapes, operands, scratch = [], [], []
    flops = moved = 0
    for tokens, basis in pairs:
        seqs, slots, features = tokens.shape
        dirs = basis.shape[1]
        count = CHUNKS if features % (CHUNKS * 128) == 0 else 1
        rows = seqs * slots
        operands += [tokens.reshape(rows, features), basis]
        shapes.append(pltpu.VMEM((rows, dirs), jnp.float32))
        scratch += [
            pltpu.VMEM((rows, features), tokens.dtype),
            pltpu.VMEM((count, features // count, dirs), basis.dtype),
            pltpu.SemaphoreType.DMA,
            pltpu.SemaphoreType.DMA((count,)),
        ]
        flops += 2 * rows * features * dirs
        moved += 2 * features * (dirs + rows)
    terms = pl.pallas_call(
        turning_kernel,
        out_shape=shapes,
        in_specs=[pl.BlockSpec(memory_space=pltpu.HBM)] * len(operands),
        out_specs=[pl.BlockSpec(memory_space=pltpu.VMEM)] * len(pairs),
        scratch_shapes=scratch,
        cost_estimate=pl.CostEstimate(flops=flops, bytes_accessed=moved, transcendentals=0),
        name="turning",
    )(*operands)
    return [
        term.reshape(tokens.shape[:2] + term.shape[1:]) for term, (tokens, _) in zip(terms, pairs)
    ]


def paired(size):
    return size & (size - 1) == 0


def source(size, own, step):
    return own ^ step if paired(size) else (own - step) % size


def target(size, own, step):
    return own ^ step if paired(size) else (own + step) % size


def sent(value, axis, step):
    size = lax.axis_size(axis)
    return lax.ppermute(value, axis, [(i, target(size, i, step)) for i in range(size)])


def every_token(turned, axis):
    pieces = [turned]
    for k in range(1, lax.axis_size(axis)):
        pieces.append(sent(turned, axis, k))
    return pieces


def summed_part(terms, axis):
    size = lax.axis_size(axis)
    own = lax.axis_index(axis)
    width = terms.shape[2] // size

    def part(owner):
        return lax.dynamic_slice_in_dim(terms, owner * width, width, 2)

    total = part(own)
    for k in range(1, size):
        total = total + sent(part(target(size, own, k)), axis, k)
    return total


def summed_whole(terms, axis):
    if lax.axis_size(axis) > 2:
        return lax.psum(terms, axis)
    return terms + sent(terms, axis, 1)


def tile_kernel(*refs, outs, ins, divisor):
    out_pieces, in_pieces = refs[:outs], refs[outs : outs + ins]
    tile_hbm, kept, turned, tile, sems = refs[outs + ins :]
    for axis, pieces, whole in (("col", out_pieces, kept), ("row", in_pieces, turned)):
        own = lax.axis_index(axis)
        for k, piece in enumerate(pieces):
            slots = piece.shape[1]
            place = pl.multiple_of(source(len(pieces), own, k) * slots, slots)
            whole[:, pl.ds(place, slots), :] = piece[...]
    steps, rows, _ = tile.shape
    writes = []
    for step in range(steps):
        total = None
        for n in range(kept.shape[0]):
            product = lax.dot_general(
                kept[n, :, step * rows : (step + 1) * rows],
                turned[n],
                (((0,), (0,)), ((), ())),
                preferred_element_type=jnp.float32,
            )
            square = product * product
            total = square if total is None else total + square
        tile[step] = total * (1.0 / divisor) if paired(divisor) else total / divisor
        write = pltpu.make_async_copy(
            tile.at[step], tile_hbm.at[pl.ds(step * rows, rows)], sems.at[step]
        )
        write.start()
        writes.append(write)
    for write in writes:
        write.wait()


def tile_of(out_pieces, in_pieces):
    seqs, out_slots, rows = out_pieces[0].shape
    cols = in_pieces[0].shape[2]
    slot_total = out_slots * len(out_pieces)
    steps = 4 if rows % 512 == 0 else 1
    dtype = out_pieces[0].dtype
    pieces = [
        pltpu.with_memory_space_constraint(piece, pltpu.VMEM) for piece in out_pieces + in_pieces
    ]
    return pl.pallas_call(
        functools.partial(
            tile_kernel, outs=len(out_pieces), ins=len(in_pieces), divisor=seqs * slot_total
        ),
        out_shape=jax.ShapeDtypeStruct((rows, cols), jnp.float32),
        in_specs=[pl.BlockSpec(memory_space=pltpu.VMEM)] * len(pieces),
        out_specs=pl.BlockSpec(memory_space=pltpu.HBM),
        scratch_shapes=[
            pltpu.VMEM((seqs, slot_total, rows), dtype),
            pltpu.VMEM((seqs, slot_total, cols), dtype),
            pltpu.VMEM((steps, rows // steps, cols), jnp.float32),
            pltpu.SemaphoreType.DMA((steps,)),
        ],
        cost_estimate=pl.CostEstimate(
            flops=2 * seqs * slot_total * rows * cols,
            bytes_accessed=4 * rows * cols,
            transcendentals=0,
        ),
        name="tile",
    )(*pieces)


def local(activations, gradients, basis_in, basis_out, lengths):
    slots = gradients.shape[1]
    out_terms, in_terms = turned_terms((gradients, basis_out), (activations, basis_in))
    turned_out = summed_part(out_terms, "seq").astype(jnp.bfloat16)
    turned_in = summed_whole(in_terms, "seq").astype(jnp.bfloat16)
    token = lax.axis_index("col") * slots + jnp.arange(slots)
    live = token[None, :] < lengths[:, None]
    kept = jnp.where(live[:, :, None], turned_out, jnp.zeros((), jnp.bfloat16))
    return tile_of(every_token(kept, "col"), every_token(turned_in, "row"))


def solution(mesh):
    return jax.shard_map(
        local,
        mesh=mesh,
        in_specs=(
            P(None, "row", "seq"),
            P(None, "col", "seq"),
            P("seq", "col"),
            P("seq", "row"),
            P(),
        ),
        out_specs=P(("row", "seq"), "col"),
        check_vma=False,
    )
```

```python
import functools

import jax
import jax.numpy as jnp
from jax import lax
from jax.experimental import pallas as pl
from jax.experimental.pallas import tpu as pltpu
from jax.sharding import PartitionSpec as P


CHUNKS = 8


def turning_kernel(*refs):
    pairs = len(refs) // 7
    sources, terms, scratch = refs[: 2 * pairs], refs[2 * pairs : 3 * pairs], refs[3 * pairs :]
    jobs = []
    for p in range(pairs):
        tokens_hbm, basis_hbm = sources[2 * p : 2 * p + 2]
        tokens, basis, token_sem, basis_sems = scratch[4 * p : 4 * p + 4]
        count, rows, _ = basis.shape
        loads = [pltpu.make_async_copy(tokens_hbm, tokens, token_sem)]
        for k in range(count):
            loads.append(
                pltpu.make_async_copy(
                    basis_hbm.at[pl.ds(k * rows, rows)], basis.at[k], basis_sems.at[k]
                )
            )
        jobs.append(loads)
    for p, loads in enumerate(jobs):
        for k, load in enumerate(loads):
            load.start(priority=int(p > 0) if pairs > 1 else int(2 * k > len(loads)))
    for p, loads in enumerate(jobs):
        tokens, basis = scratch[4 * p : 4 * p + 2]
        count, rows, _ = basis.shape
        loads[0].wait()
        total = None
        for k in range(count):
            loads[k + 1].wait()
            part = jnp.dot(
                tokens[:, k * rows : (k + 1) * rows], basis[k], preferred_element_type=jnp.float32
            )
            total = part if total is None else total + part
        terms[p][...] = total


def turned_terms(*pairs):
    shapes, operands, scratch = [], [], []
    flops = moved = 0
    for tokens, basis in pairs:
        seqs, slots, features = tokens.shape
        dirs = basis.shape[1]
        count = CHUNKS if features % (CHUNKS * 128) == 0 else 1
        rows = seqs * slots
        operands += [
            pltpu.with_memory_space_constraint(array, pltpu.HBM)
            for array in (tokens.reshape(rows, features), basis)
        ]
        shapes.append(pltpu.VMEM((rows, dirs), jnp.float32))
        scratch += [
            pltpu.VMEM((rows, features), tokens.dtype),
            pltpu.VMEM((count, features // count, dirs), basis.dtype),
            pltpu.SemaphoreType.DMA,
            pltpu.SemaphoreType.DMA((count,)),
        ]
        flops += 2 * rows * features * dirs
        moved += 2 * features * (dirs + rows)
    terms = pl.pallas_call(
        turning_kernel,
        out_shape=shapes,
        in_specs=[pl.BlockSpec(memory_space=pltpu.HBM)] * len(operands),
        out_specs=[pl.BlockSpec(memory_space=pltpu.VMEM)] * len(pairs),
        scratch_shapes=scratch,
        cost_estimate=pl.CostEstimate(flops=flops, bytes_accessed=moved, transcendentals=0),
        compiler_params=pltpu.CompilerParams(vmem_limit_bytes=24 << 20),
        name="turning",
    )(*operands)
    return [
        term.reshape(tokens.shape[:2] + term.shape[1:]) for term, (tokens, _) in zip(terms, pairs)
    ]


def held_kernel(tokens, basis, terms):
    terms[...] = jnp.dot(tokens[...], basis[...], preferred_element_type=jnp.float32)


def held_terms(tokens, basis):
    seqs, slots, features = tokens.shape
    dirs = basis.shape[1]
    rows = seqs * slots
    terms = pl.pallas_call(
        held_kernel,
        out_shape=pltpu.VMEM((rows, dirs), jnp.float32),
        in_specs=[pl.BlockSpec(memory_space=pltpu.VMEM)] * 2,
        out_specs=pl.BlockSpec(memory_space=pltpu.VMEM),
        cost_estimate=pl.CostEstimate(
            flops=2 * rows * features * dirs, bytes_accessed=4 * rows * dirs, transcendentals=0
        ),
        compiler_params=pltpu.CompilerParams(vmem_limit_bytes=24 << 20),
        name="held",
    )(
        pltpu.with_memory_space_constraint(tokens.reshape(rows, features), pltpu.VMEM),
        pltpu.with_memory_space_constraint(basis, pltpu.VMEM),
    )
    return terms.reshape(seqs, slots, dirs)


def paired(size):
    return size & (size - 1) == 0


def source(size, own, step):
    return own ^ step if paired(size) else (own - step) % size


def target(size, own, step):
    return own ^ step if paired(size) else (own + step) % size


def sent(value, axis, step):
    size = lax.axis_size(axis)
    return lax.ppermute(value, axis, [(i, target(size, i, step)) for i in range(size)])


def every_token(turned, axis):
    pieces = [turned]
    for k in range(1, lax.axis_size(axis)):
        pieces.append(sent(turned, axis, k))
    return pieces


def summed_part(terms, axis):
    size = lax.axis_size(axis)
    own = lax.axis_index(axis)
    width = terms.shape[2] // size

    def part(owner):
        return lax.dynamic_slice_in_dim(terms, owner * width, width, 2)

    total = part(own)
    for k in range(1, size):
        total = total + sent(part(target(size, own, k)), axis, k)
    return total


def summed_whole(terms, axis):
    if lax.axis_size(axis) > 2:
        return lax.psum(terms, axis)
    return terms + sent(terms, axis, 1)


def tile_kernel(*refs, outs, ins, divisor):
    out_pieces, in_pieces = refs[:outs], refs[outs : outs + ins]
    tile_hbm, kept, turned, tile, sems = refs[outs + ins :]
    for axis, pieces, whole in (("col", out_pieces, kept), ("row", in_pieces, turned)):
        own = lax.axis_index(axis)
        for k, piece in enumerate(pieces):
            slots = piece.shape[1]
            place = pl.multiple_of(source(len(pieces), own, k) * slots, slots)
            whole[:, pl.ds(place, slots), :] = piece[...]
    steps, rows, _ = tile.shape
    writes = []
    for step in range(steps):
        total = None
        for n in range(kept.shape[0]):
            product = lax.dot_general(
                kept[n, :, step * rows : (step + 1) * rows],
                turned[n],
                (((0,), (0,)), ((), ())),
                preferred_element_type=jnp.float32,
            )
            square = product * product
            total = square if total is None else total + square
        tile[step] = total * (1.0 / divisor) if paired(divisor) else total / divisor
        write = pltpu.make_async_copy(
            tile.at[step], tile_hbm.at[pl.ds(step * rows, rows)], sems.at[step]
        )
        write.start()
        writes.append(write)
    for write in writes:
        write.wait()


def tile_of(out_pieces, in_pieces):
    seqs, out_slots, rows = out_pieces[0].shape
    cols = in_pieces[0].shape[2]
    slot_total = out_slots * len(out_pieces)
    steps = 4 if rows % 512 == 0 else 1
    dtype = out_pieces[0].dtype
    pieces = [
        pltpu.with_memory_space_constraint(piece, pltpu.VMEM) for piece in out_pieces + in_pieces
    ]
    return pl.pallas_call(
        functools.partial(
            tile_kernel, outs=len(out_pieces), ins=len(in_pieces), divisor=seqs * slot_total
        ),
        out_shape=jax.ShapeDtypeStruct((rows, cols), jnp.float32),
        in_specs=[pl.BlockSpec(memory_space=pltpu.VMEM)] * len(pieces),
        out_specs=pl.BlockSpec(memory_space=pltpu.HBM),
        scratch_shapes=[
            pltpu.VMEM((seqs, slot_total, rows), dtype),
            pltpu.VMEM((seqs, slot_total, cols), dtype),
            pltpu.VMEM((steps, rows // steps, cols), jnp.float32),
            pltpu.SemaphoreType.DMA((steps,)),
        ],
        cost_estimate=pl.CostEstimate(
            flops=2 * seqs * slot_total * rows * cols,
            bytes_accessed=4 * rows * cols,
            transcendentals=0,
        ),
        name="tile",
    )(*pieces)


def local(activations, gradients, basis_in, basis_out, lengths):
    slots = gradients.shape[1]
    (out_terms,) = turned_terms((gradients, basis_out))
    in_terms = held_terms(activations, basis_in)
    turned_out = summed_part(out_terms, "seq").astype(jnp.bfloat16)
    turned_in = summed_whole(in_terms, "seq").astype(jnp.bfloat16)
    token = lax.axis_index("col") * slots + jnp.arange(slots)
    live = token[None, :] < lengths[:, None]
    kept = jnp.where(live[:, :, None], turned_out, jnp.zeros((), jnp.bfloat16))
    return tile_of(every_token(kept, "col"), every_token(turned_in, "row"))


def solution(mesh):
    return jax.shard_map(
        local,
        mesh=mesh,
        in_specs=(
            P(None, "row", "seq"),
            P(None, "col", "seq"),
            P("seq", "col"),
            P("seq", "row"),
            P(),
        ),
        out_specs=P(("row", "seq"), "col"),
        check_vma=False,
    )
```

```python
import functools

import jax
import jax.numpy as jnp
from jax import lax
from jax.experimental import pallas as pl
from jax.experimental.pallas import tpu as pltpu
from jax.sharding import PartitionSpec as P


CHUNKS = (2, 2, 2, 1, 1, 1, 1, 1, 1, 1, 1, 1, 1)
AHEAD = 3


def turning_kernel(tokens_hbm, basis_hbm, terms, tokens, basis, token_sem, sems, *, spans, ahead):
    load = pltpu.make_async_copy(tokens_hbm, tokens, token_sem)
    load.start()
    chunks = []
    for k, span in enumerate(spans):
        rows = pl.ds(sum(spans[:k]), span)
        chunks.append(pltpu.make_async_copy(basis_hbm.at[rows], basis.at[rows], sems.at[k]))
        chunks[k].start(priority=int(k >= ahead))
    load.wait()
    total = None
    for k, span in enumerate(spans):
        chunks[k].wait()
        first = sum(spans[:k])
        part = jnp.dot(
            tokens[:, first : first + span],
            basis[first : first + span],
            preferred_element_type=jnp.float32,
        )
        total = part if total is None else total + part
    terms[...] = total


def turned_terms(tokens, basis):
    seqs, slots, features = tokens.shape
    dirs = basis.shape[1]
    rows = seqs * slots
    unit = features // sum(CHUNKS)
    spans = [unit * c for c in CHUNKS] if unit % 128 == 0 and unit else [features]
    terms = pl.pallas_call(
        functools.partial(turning_kernel, spans=spans, ahead=AHEAD),
        out_shape=pltpu.VMEM((rows, dirs), jnp.float32),
        in_specs=[pl.BlockSpec(memory_space=pltpu.HBM)] * 2,
        out_specs=pl.BlockSpec(memory_space=pltpu.VMEM),
        scratch_shapes=[
            pltpu.VMEM((rows, features), tokens.dtype),
            pltpu.VMEM((features, dirs), basis.dtype),
            pltpu.SemaphoreType.DMA,
            pltpu.SemaphoreType.DMA((len(spans),)),
        ],
        cost_estimate=pl.CostEstimate(
            flops=2 * rows * features * dirs,
            bytes_accessed=2 * features * (dirs + rows),
            transcendentals=0,
        ),
        compiler_params=pltpu.CompilerParams(vmem_limit_bytes=24 << 20),
        name="turning",
    )(
        pltpu.with_memory_space_constraint(tokens.reshape(rows, features), pltpu.HBM),
        pltpu.with_memory_space_constraint(basis, pltpu.HBM),
    )
    return terms.reshape(seqs, slots, dirs)


def held_kernel(tokens, basis, terms):
    terms[...] = jnp.dot(tokens[...], basis[...], preferred_element_type=jnp.float32)


def held_terms(tokens, basis):
    seqs, slots, features = tokens.shape
    dirs = basis.shape[1]
    rows = seqs * slots
    terms = pl.pallas_call(
        held_kernel,
        out_shape=pltpu.VMEM((rows, dirs), jnp.float32),
        in_specs=[pl.BlockSpec(memory_space=pltpu.VMEM)] * 2,
        out_specs=pl.BlockSpec(memory_space=pltpu.VMEM),
        cost_estimate=pl.CostEstimate(
            flops=2 * rows * features * dirs, bytes_accessed=4 * rows * dirs, transcendentals=0
        ),
        compiler_params=pltpu.CompilerParams(vmem_limit_bytes=24 << 20),
        name="held",
    )(
        pltpu.with_memory_space_constraint(tokens.reshape(rows, features), pltpu.VMEM),
        pltpu.with_memory_space_constraint(basis, pltpu.VMEM),
    )
    return terms.reshape(seqs, slots, dirs)


def paired(size):
    return size & (size - 1) == 0


def source(size, own, step):
    return own ^ step if paired(size) else (own - step) % size


def target(size, own, step):
    return own ^ step if paired(size) else (own + step) % size


def sent(value, axis, step):
    size = lax.axis_size(axis)
    return lax.ppermute(value, axis, [(i, target(size, i, step)) for i in range(size)])


def every_token(turned, axis):
    pieces = [turned]
    for k in range(1, lax.axis_size(axis)):
        pieces.append(sent(turned, axis, k))
    return pieces


def every_token_by_pairs(turned, axis):
    size = lax.axis_size(axis)
    if size % 2 or not paired(size):
        return every_token(turned, axis)
    pieces = []
    for k in range(0, size, 2):
        far = turned
        if k:
            far = sent(turned, axis, k)
        pieces += [far, sent(far, axis, 1)]
    return pieces


def summed_part(terms, axis):
    size = lax.axis_size(axis)
    own = lax.axis_index(axis)
    width = terms.shape[2] // size

    def part(owner):
        return lax.dynamic_slice_in_dim(terms, owner * width, width, 2)

    total = part(own)
    for k in range(1, size):
        total = total + sent(part(target(size, own, k)), axis, k)
    return total


def summed_whole(terms, axis):
    if lax.axis_size(axis) > 2:
        return lax.psum(terms, axis)
    return terms + sent(terms, axis, 1)


def tile_kernel(*refs, outs, ins, divisor):
    out_pieces, in_pieces = refs[:outs], refs[outs : outs + ins]
    tile_hbm, kept, turned, tile, sems = refs[outs + ins :]
    for axis, pieces, whole in (("col", out_pieces, kept), ("row", in_pieces, turned)):
        own = lax.axis_index(axis)
        for k, piece in enumerate(pieces):
            slots = piece.shape[1]
            place = pl.multiple_of(source(len(pieces), own, k) * slots, slots)
            whole[:, pl.ds(place, slots), :] = piece[...]
    steps, rows, _ = tile.shape
    writes = []
    for step in range(steps):
        total = None
        for n in range(kept.shape[0]):
            product = lax.dot_general(
                kept[n, :, step * rows : (step + 1) * rows],
                turned[n],
                (((0,), (0,)), ((), ())),
                preferred_element_type=jnp.float32,
            )
            square = product * product
            total = square if total is None else total + square
        tile[step] = total * (1.0 / divisor) if paired(divisor) else total / divisor
        write = pltpu.make_async_copy(
            tile.at[step], tile_hbm.at[pl.ds(step * rows, rows)], sems.at[step]
        )
        write.start()
        writes.append(write)
    for write in writes:
        write.wait()


def tile_of(out_pieces, in_pieces):
    seqs, out_slots, rows = out_pieces[0].shape
    cols = in_pieces[0].shape[2]
    slot_total = out_slots * len(out_pieces)
    steps = 4 if rows % 512 == 0 else 1
    dtype = out_pieces[0].dtype
    pieces = [
        pltpu.with_memory_space_constraint(piece, pltpu.VMEM) for piece in out_pieces + in_pieces
    ]
    return pl.pallas_call(
        functools.partial(
            tile_kernel, outs=len(out_pieces), ins=len(in_pieces), divisor=seqs * slot_total
        ),
        out_shape=jax.ShapeDtypeStruct((rows, cols), jnp.float32),
        in_specs=[pl.BlockSpec(memory_space=pltpu.VMEM)] * len(pieces),
        out_specs=pl.BlockSpec(memory_space=pltpu.HBM),
        scratch_shapes=[
            pltpu.VMEM((seqs, slot_total, rows), dtype),
            pltpu.VMEM((seqs, slot_total, cols), dtype),
            pltpu.VMEM((steps, rows // steps, cols), jnp.float32),
            pltpu.SemaphoreType.DMA((steps,)),
        ],
        cost_estimate=pl.CostEstimate(
            flops=2 * seqs * slot_total * rows * cols,
            bytes_accessed=4 * rows * cols,
            transcendentals=0,
        ),
        name="tile",
    )(*pieces)


def local(activations, gradients, basis_in, basis_out, lengths):
    slots = gradients.shape[1]
    out_terms = turned_terms(gradients, basis_out)
    in_terms = held_terms(activations, basis_in)
    turned_out = summed_part(out_terms, "seq").astype(jnp.bfloat16)
    turned_in = summed_whole(in_terms, "seq").astype(jnp.bfloat16)
    token = lax.axis_index("col") * slots + jnp.arange(slots)
    live = token[None, :] < lengths[:, None]
    kept = jnp.where(live[:, :, None], turned_out, jnp.zeros((), jnp.bfloat16))
    return tile_of(every_token(kept, "col"), every_token_by_pairs(turned_in, "row"))


def solution(mesh):
    return jax.shard_map(
        local,
        mesh=mesh,
        in_specs=(
            P(None, "row", "seq"),
            P(None, "col", "seq"),
            P("seq", "col"),
            P("seq", "row"),
            P(),
        ),
        out_specs=P(("row", "seq"), "col"),
        check_vma=False,
    )
```

```python
import functools

import jax
import jax.numpy as jnp
from jax import lax
from jax.experimental import pallas as pl
from jax.experimental.pallas import tpu as pltpu
from jax.sharding import PartitionSpec as P


CHUNKS = (2, 2, 2, 1, 1, 1, 1, 1, 1, 1, 1, 1, 1)
AHEAD = 3


def turning_kernel(tokens_hbm, basis_hbm, terms, tokens, basis, token_sem, sems, *, spans, ahead):
    load = pltpu.make_async_copy(tokens_hbm, tokens, token_sem)
    load.start()
    chunks = []
    for k, span in enumerate(spans):
        rows = pl.ds(sum(spans[:k]), span)
        chunks.append(pltpu.make_async_copy(basis_hbm.at[rows], basis.at[rows], sems.at[k]))
        chunks[k].start(priority=int(k >= ahead))
    load.wait()
    total = None
    for k, span in enumerate(spans):
        chunks[k].wait()
        first = sum(spans[:k])
        part = jnp.dot(
            tokens[:, first : first + span],
            basis[first : first + span],
            preferred_element_type=jnp.float32,
        )
        total = part if total is None else total + part
    terms[...] = total


def turned_terms(tokens, basis):
    seqs, slots, features = tokens.shape
    dirs = basis.shape[1]
    rows = seqs * slots
    unit = features // sum(CHUNKS)
    spans = [unit * c for c in CHUNKS] if unit % 128 == 0 and unit else [features]
    terms = pl.pallas_call(
        functools.partial(turning_kernel, spans=spans, ahead=AHEAD),
        out_shape=pltpu.VMEM((rows, dirs), jnp.float32),
        in_specs=[pl.BlockSpec(memory_space=pltpu.HBM)] * 2,
        out_specs=pl.BlockSpec(memory_space=pltpu.VMEM),
        scratch_shapes=[
            pltpu.VMEM((rows, features), tokens.dtype),
            pltpu.VMEM((features, dirs), basis.dtype),
            pltpu.SemaphoreType.DMA,
            pltpu.SemaphoreType.DMA((len(spans),)),
        ],
        cost_estimate=pl.CostEstimate(
            flops=2 * rows * features * dirs,
            bytes_accessed=2 * features * (dirs + rows),
            transcendentals=0,
        ),
        compiler_params=pltpu.CompilerParams(vmem_limit_bytes=24 << 20),
        name="turning",
    )(
        pltpu.with_memory_space_constraint(tokens.reshape(rows, features), pltpu.HBM),
        pltpu.with_memory_space_constraint(basis, pltpu.HBM),
    )
    return terms.reshape(seqs, slots, dirs)


def held_kernel(tokens, basis, terms):
    terms[...] = jnp.dot(tokens[...], basis[...], preferred_element_type=jnp.float32)


def held_terms(tokens, basis):
    seqs, slots, features = tokens.shape
    dirs = basis.shape[1]
    rows = seqs * slots
    terms = pl.pallas_call(
        held_kernel,
        out_shape=pltpu.VMEM((rows, dirs), jnp.float32),
        in_specs=[pl.BlockSpec(memory_space=pltpu.VMEM)] * 2,
        out_specs=pl.BlockSpec(memory_space=pltpu.VMEM),
        cost_estimate=pl.CostEstimate(
            flops=2 * rows * features * dirs, bytes_accessed=4 * rows * dirs, transcendentals=0
        ),
        compiler_params=pltpu.CompilerParams(vmem_limit_bytes=24 << 20),
        name="held",
    )(
        pltpu.with_memory_space_constraint(tokens.reshape(rows, features), pltpu.VMEM),
        pltpu.with_memory_space_constraint(basis, pltpu.VMEM),
    )
    return terms.reshape(seqs, slots, dirs)


def paired(size):
    return size & (size - 1) == 0


def source(size, own, step):
    return own ^ step if paired(size) else (own - step) % size


def target(size, own, step):
    return own ^ step if paired(size) else (own + step) % size


def sent(value, axis, step):
    size = lax.axis_size(axis)
    return lax.ppermute(value, axis, [(i, target(size, i, step)) for i in range(size)])


def every_token(turned, axis):
    pieces = [turned]
    for k in range(1, lax.axis_size(axis)):
        pieces.append(sent(turned, axis, k))
    return pieces


def every_token_by_pairs(turned, axis):
    size = lax.axis_size(axis)
    if size % 2 or not paired(size):
        return every_token(turned, axis)
    pieces = []
    for k in range(0, size, 2):
        far = turned
        if k:
            far = sent(turned, axis, k)
        pieces += [far, sent(far, axis, 1)]
    return pieces


def summed_part(terms, axis):
    size = lax.axis_size(axis)
    own = lax.axis_index(axis)
    width = terms.shape[2] // size

    def part(owner):
        return lax.dynamic_slice_in_dim(terms, owner * width, width, 2)

    total = part(own)
    for k in range(1, size):
        total = total + sent(part(target(size, own, k)), axis, k)
    return total


def summed_whole(terms, axis):
    if lax.axis_size(axis) > 2:
        return lax.psum(terms, axis)
    return terms + sent(terms, axis, 1)


def tile_kernel(*refs, outs, ins, divisor, spans):
    out_pieces, in_pieces = refs[:outs], refs[outs : outs + ins]
    tile_hbm, kept, turned, tile, sems = refs[outs + ins :]
    for axis, pieces, whole in (("col", out_pieces, kept), ("row", in_pieces, turned)):
        own = lax.axis_index(axis)
        for k, piece in enumerate(pieces):
            slots = piece.shape[1]
            place = pl.multiple_of(source(len(pieces), own, k) * slots, slots)
            whole[:, pl.ds(place, slots), :] = piece[...]
    writes = []
    first = 0
    for step, rows in enumerate(spans):
        place = slice(first, first + rows)
        total = None
        for n in range(kept.shape[0]):
            product = lax.dot_general(
                kept[n, :, place],
                turned[n],
                (((0,), (0,)), ((), ())),
                preferred_element_type=jnp.float32,
            )
            square = product * product
            total = square if total is None else total + square
        tile[place] = total * (1.0 / divisor) if paired(divisor) else total / divisor
        write = pltpu.make_async_copy(
            tile.at[pl.ds(first, rows)], tile_hbm.at[pl.ds(first, rows)], sems.at[step]
        )
        write.start(priority=step % 2)
        writes.append(write)
        first += rows
    for write in writes:
        write.wait()


def tile_of(out_pieces, in_pieces):
    seqs, out_slots, rows = out_pieces[0].shape
    cols = in_pieces[0].shape[2]
    slot_total = out_slots * len(out_pieces)
    spans = [rows // 8] * 8 if rows % 512 == 0 else [rows]
    dtype = out_pieces[0].dtype
    pieces = [
        pltpu.with_memory_space_constraint(piece, pltpu.VMEM) for piece in out_pieces + in_pieces
    ]
    return pl.pallas_call(
        functools.partial(
            tile_kernel, outs=len(out_pieces), ins=len(in_pieces), divisor=seqs * slot_total, spans=spans
        ),
        out_shape=jax.ShapeDtypeStruct((rows, cols), jnp.float32),
        in_specs=[pl.BlockSpec(memory_space=pltpu.VMEM)] * len(pieces),
        out_specs=pl.BlockSpec(memory_space=pltpu.HBM),
        scratch_shapes=[
            pltpu.VMEM((seqs, slot_total, rows), dtype),
            pltpu.VMEM((seqs, slot_total, cols), dtype),
            pltpu.VMEM((rows, cols), jnp.float32),
            pltpu.SemaphoreType.DMA((len(spans),)),
        ],
        cost_estimate=pl.CostEstimate(
            flops=2 * seqs * slot_total * rows * cols,
            bytes_accessed=4 * rows * cols,
            transcendentals=0,
        ),
        name="tile",
    )(*pieces)


def local(activations, gradients, basis_in, basis_out, lengths):
    slots = gradients.shape[1]
    out_terms = turned_terms(gradients, basis_out)
    in_terms = held_terms(activations, basis_in)
    turned_out = summed_part(out_terms, "seq").astype(jnp.bfloat16)
    turned_in = summed_whole(in_terms, "seq").astype(jnp.bfloat16)
    token = lax.axis_index("col") * slots + jnp.arange(slots)
    live = token[None, :] < lengths[:, None]
    kept = jnp.where(live[:, :, None], turned_out, jnp.zeros((), jnp.bfloat16))
    return tile_of(every_token(kept, "col"), every_token_by_pairs(turned_in, "row"))


def solution(mesh):
    return jax.shard_map(
        local,
        mesh=mesh,
        in_specs=(
            P(None, "row", "seq"),
            P(None, "col", "seq"),
            P("seq", "col"),
            P("seq", "row"),
            P(),
        ),
        out_specs=P(("row", "seq"), "col"),
        check_vma=False,
    )
```
